32 devices in a mesh: gx: 4 (over z), gy: 4 (over x, core), gz: 2 (over y).
Axes of the slice: x: 2, y: 2, z: 4, core: 2. Of those that a mesh axis runs over, the one named last changes fastest.
Arguments:
- volume: int32 [32, 64, 256], P('gx', 'gy', 'gz'), may hold values from 0 to 255
- transfer_table: float32 [4, 256], replicated, may hold values from 0 to 1
- depth_rank: int32 [4], replicated, may hold values from 0 to 3, each once
- footprint: int32 [4, 4, 2, 4], P('gx', 'gy', 'gz'), may hold values from 0 to 128, as said below
Outputs:
- rendered: float32 [4, 64, 256], P(None, 'gy', 'gz')
The draws below stay inside these ranges and needn't reach their ends.
Inputs may be any that keep to these rules, and one draw needn't show every extreme that they name: depth_rank holds each of 0 to 4 - 1 once. `footprint`: for every brick, entry 0 is below 8 and entry 1 above it, up to 16; entry 2 is below 64 and entry 3 above it, up to 128.
All inputs are finite; a program needn't handle non-finite values.
Results may differ from the reference program's by a relative error of at most 0.0003.
Values sent between devices are 32-bit elements; how exact they have to be, the bound alone decides.
No kernel may reach another device: no remote copies, remote signals or barrier semaphores. Data moves between devices by JAX's collectives and lax.ppermute only.
A program may use at most 64 MiB of HBM per device.

```python
import jax
import jax.numpy as jnp
from jax import lax

CX = 8
CY = 16
CZ = 128
TF = 256
NX = 32
NY = 64
NZ = 256
N_GX = 4
N_GY = 4
N_GZ = 2


def draw_footprint(key, part):
    keys = jax.random.split(jax.random.fold_in(key, 7), 4)
    shaped = (N_GX, N_GY, N_GZ)
    first_row = jax.random.randint(keys[0], shaped, 0, CY // 2)
    end_row = jax.random.randint(keys[1], shaped, CY // 2 + 1, CY + 1)
    first_col = jax.random.randint(keys[2], shaped, 0, CZ // 2)
    end_col = jax.random.randint(keys[3], shaped, CZ // 2 + 1, CZ + 1)
    return jnp.stack([first_row, end_row, first_col, end_col], axis=-1).astype(jnp.int32)


def with_ends(result, stream_key, least, high):
    longest = result.shape.index(max(result.shape))
    spots = []
    for shift in (0, 1):
        where = [jax.random.randint(jax.random.fold_in(stream_key, axis), (), 0, length) for axis, length in enumerate(result.shape)]
        where[longest] = (where[longest] + shift) % result.shape[longest]
        spots.append(tuple(where))
    return result.at[spots[0]].set(least).at[spots[1]].set(high)


def setup_inputs(seed: int = 0) -> dict:
    key_list = jax.random.split(jax.random.key(seed), 5)
    return {
        "volume": with_ends(jax.random.randint(key_list[0], (NX, NY, NZ), 0, TF), jax.random.fold_in(key_list[0], 1), 0, TF - 1).astype(jnp.int32),
        "transfer_table": jnp.clip(jax.random.uniform(key_list[1], (4, TF), jnp.float32, 0.0, 1.0), 0.0, 1.0),
        "depth_rank": jax.random.permutation(key_list[2], N_GX).astype(jnp.int32),
        "footprint": draw_footprint(jax.random.fold_in(key_list[4], 71), 0),
    }


light_x = 1.0 / 3.0
light_y = 2.0 / 3.0
light_z = 2.0 / 3.0

def shading(lower_plane, upper_plane, padded):
    grad_x = 0.5 * (upper_plane - lower_plane)
    grad_y = 0.5 * (padded[2:, 1:-1] - padded[:-2, 1:-1])
    grad_z = 0.5 * (padded[1:-1, 2:] - padded[1:-1, :-2])
    facing = jnp.abs(grad_x * light_x + grad_y * light_y + grad_z * light_z) / jnp.sqrt(1.0 + (grad_x * grad_x + grad_y * grad_y + grad_z * grad_z))
    return 0.35 + 0.65 * facing

def composite(layers, depth_rank):
    order = jnp.argsort(depth_rank).astype(jnp.int32)
    ordered = jnp.take(layers, order, axis=0)

    def blend(state_pair, front_layer):
        colour, alpha = state_pair
        cover = 1.0 - alpha
        return ((colour + cover * front_layer[:3], alpha + cover * front_layer[3]), None)
    start_pair = (jnp.zeros((3,) + layers.shape[2:], jnp.float32), jnp.zeros(layers.shape[2:], jnp.float32))
    (colour, alpha), unused = lax.scan(blend, start_pair, ordered)
    return jnp.concatenate([colour, alpha[None]], axis=0)

def reference(volume, transfer_table, depth_rank, footprint):
    opacity = transfer_table[3]
    colors = transfer_table[:3]
    extent = 4.0 / NX

    def density(slice_at):
        inside = ((slice_at >= 0) & (slice_at < NX)).astype(jnp.float32)
        clipped = jnp.clip(slice_at, 0, NX - 1).astype(jnp.int32)
        indices = lax.dynamic_index_in_dim(volume, clipped, 0, keepdims=False)
        return (jnp.take(opacity, indices, axis=0) * inside, indices)

    def advance(state_pair, slice_at):
        colour, transmit = state_pair
        centre, indices = density(slice_at)
        lower_plane, unused_low = density(slice_at - 1)
        upper_plane, unused_high = density(slice_at + 1)
        shading_term = shading(lower_plane, upper_plane, jnp.pad(centre, 1))
        emitted = jnp.take(colors, indices, axis=1) * shading_term
        sample_alpha = 1.0 - jnp.exp(-extent * centre)
        colour = colour + transmit * sample_alpha * emitted
        transmit = transmit * (1.0 - sample_alpha)
        return ((colour, transmit), None)
    rows_local = (jnp.arange(NY, dtype=jnp.int32) % CY)[:, None]
    cols_local = (jnp.arange(NZ, dtype=jnp.int32) % CZ)[None, :]
    partials = []
    for column in range(N_GX):
        start_pair = (jnp.zeros((3, NY, NZ), jnp.float32), jnp.ones((NY, NZ), jnp.float32))
        slices_here = jnp.arange(CX, dtype=jnp.int32) + column * CX
        (colour, transmit), unused = lax.scan(advance, start_pair, slices_here)
        rect = jnp.repeat(jnp.repeat(footprint[column], CY, axis=0), CZ, axis=1)
        inside = (rows_local >= rect[..., 0]) & (rows_local < rect[..., 1]) & (cols_local >= rect[..., 2]) & (cols_local < rect[..., 3])
        layer = jnp.concatenate([colour, (1.0 - transmit)[None]], axis=0)
        partials.append(jnp.where(inside[None], layer, 0.0))
    return composite(jnp.stack(partials), depth_rank)
```

```python
import functools

import jax
import jax.numpy as jnp
from jax import lax
from jax.experimental import pallas as pl
from jax.experimental.pallas import tpu as pltpu
from jax.sharding import PartitionSpec as P

AXES = ("gx", "gy", "gz")
LANES = 128
LIGHT = (1.0 / 3.0, 2.0 / 3.0, 2.0 / 3.0)
SMALL_VMEM = 4 * 1024 * 1024


def partner(index, count, step):
    other = index + 1 if index % 2 == step else index - 1
    return other if 0 <= other < count else None


def swap_pairs(sizes, axis, step):
    pairs = []
    for x in range(sizes[0]):
        for y in range(sizes[1]):
            for z in range(sizes[2]):
                here = [x, y, z]
                there = list(here)
                other = partner(here[axis], sizes[axis], step)
                if other is not None:
                    there[axis] = other
                elif axis == 1 and sizes[1] % 2 == 0:
                    there[1] = sizes[1] - 1 - y
                elif axis != 1 and sizes[1] % 2 == 0:
                    there[1] = y ^ 1
                flat = [(a * sizes[1] + b) * sizes[2] + c for a, b, c in (here, there)]
                pairs.append(tuple(flat))
    return pairs


def swaps_of(sizes):
    return [(axis, step) for axis in range(3) for step in range(2) if sizes[axis] > 1 + step]


def is_even(axis):
    return lax.rem(lax.axis_index(AXES[axis]), 2) == 0


def pack_kernel(swaps, volume, *messages):
    depth, rows, cols = volume.shape
    lane = lax.broadcasted_iota(jnp.int32, (rows, cols), 1)
    for (axis, step), message in zip(swaps, messages):
        send_high = is_even(axis) if step == 0 else jnp.logical_not(is_even(axis))
        if axis == 0:
            message[...] = volume[jnp.where(send_high, depth - 1, 0)]
        elif axis == 1:
            message[...] = jnp.where(send_high, volume[:, rows - 1, :], volume[:, 0, :])
        else:
            packed = jnp.zeros((rows, cols), jnp.int32)
            for d in range(depth):
                shift = jnp.where(send_high, d + 1, d)
                packed = jnp.where(lane == d, pltpu.roll(volume[d], shift, 1), packed)
            message[...] = packed


def looked_up(table, channel, indices):
    rows = indices.shape[0]
    low = lax.rem(indices, LANES)
    result = None
    for start in range(0, table.shape[1], LANES):
        piece = jnp.broadcast_to(table[channel : channel + 1, start : start + LANES], (rows, LANES))
        found = jnp.take_along_axis(piece, low, axis=1, mode="promise_in_bounds")
        result = found if result is None else jnp.where(indices >= start, found, result)
    return result


def march_kernel(swaps, sizes, extent, volume, table, footprint, *refs):
    messages, partial = refs[:-1], refs[-1]
    depth, rows, cols = volume.shape
    lane = lax.broadcasted_iota(jnp.int32, (rows, cols), 1)
    row = lax.broadcasted_iota(jnp.int32, (rows, cols), 0)

    below = [jnp.zeros((rows, cols), jnp.float32), jnp.zeros((depth, cols), jnp.float32), jnp.zeros((rows, cols), jnp.float32)]
    above = list(below)
    for (axis, step), message in zip(swaps, messages):
        index = lax.axis_index(AXES[axis])
        neighbour_above = is_even(axis) if step == 0 else jnp.logical_not(is_even(axis))
        other = jnp.where(neighbour_above, index + 1, index - 1)
        present = (other >= 0) & (other < sizes[axis])
        found = looked_up(table, 3, message[...])
        above[axis] = jnp.where(neighbour_above & present, found, above[axis])
        below[axis] = jnp.where(jnp.logical_not(neighbour_above) & present, found, below[axis])

    density = [looked_up(table, 3, volume[d]) for d in range(depth)]
    colour = [jnp.zeros((rows, cols), jnp.float32) for _ in range(3)]
    transmit = jnp.ones((rows, cols), jnp.float32)
    for d in range(depth):
        centre = density[d]
        low = density[d - 1] if d > 0 else below[0]
        high = density[d + 1] if d < depth - 1 else above[0]
        grad_x = 0.5 * (high - low)
        low = jnp.where(row == 0, below[1][d : d + 1, :], pltpu.roll(centre, 1, 0))
        high = jnp.where(row == rows - 1, above[1][d : d + 1, :], pltpu.roll(centre, rows - 1, 0))
        grad_y = 0.5 * (high - low)
        low = jnp.where(lane == 0, pltpu.roll(below[2], (cols - d) % cols, 1), pltpu.roll(centre, 1, 1))
        high = jnp.where(lane == cols - 1, pltpu.roll(above[2], cols - 1 - d, 1), pltpu.roll(centre, cols - 1, 1))
        grad_z = 0.5 * (high - low)
        dot = grad_x * LIGHT[0] + grad_y * LIGHT[1] + grad_z * LIGHT[2]
        norm = 1.0 + (grad_x * grad_x + grad_y * grad_y + grad_z * grad_z)
        shading = 0.35 + 0.65 * (jnp.abs(dot) * lax.rsqrt(norm))
        sample_alpha = 1.0 - jnp.exp(-extent * centre)
        weight = transmit * sample_alpha * shading
        for c in range(3):
            colour[c] = colour[c] + weight * looked_up(table, c, volume[d])
        transmit = transmit * (1.0 - sample_alpha)

    inside = (row >= footprint[0]) & (row < footprint[1]) & (lane >= footprint[2]) & (lane < footprint[3])
    for c in range(3):
        partial[c] = jnp.where(inside, colour[c], 0.0)
    partial[3] = jnp.where(inside, transmit, 1.0)


def blend_kernel(count, ranks, *refs):
    layers, out = refs[:-1], refs[-1]
    me = lax.axis_index(AXES[0])
    rank = [ranks[lax.rem(me + k, count)] for k in range(count)]
    transmit = [layer[3] for layer in layers]
    colour = [jnp.zeros(transmit[0].shape, jnp.float32) for _ in range(3)]
    for i in range(count):
        cover = jnp.ones(transmit[0].shape, jnp.float32)
        for j in range(count):
            if j != i:
                cover = cover * jnp.where(rank[j] < rank[i], transmit[j], 1.0)
        for c in range(3):
            colour[c] = colour[c] + cover * layers[i][c]
    through = functools.reduce(lambda a, b: a * b, transmit)
    for c in range(3):
        out[c] = colour[c]
    out[3] = 1.0 - through


VMEM = pl.BlockSpec(memory_space=pltpu.VMEM)
SMEM = pl.BlockSpec(memory_space=pltpu.SMEM)
PARAMS = pltpu.CompilerParams(vmem_limit_bytes=SMALL_VMEM)


def cost(flops):
    return pl.CostEstimate(flops=flops, bytes_accessed=1 << 16, transcendentals=0)


def on_device(volume, transfer_table, depth_rank, footprint):
    depth, rows, cols = volume.shape
    sizes = tuple(lax.axis_size(name) for name in AXES)
    extent = 4.0 / (depth * sizes[0])
    swaps = swaps_of(sizes)

    shapes = [(depth, cols) if axis == 1 else (rows, cols) for axis, _ in swaps]
    messages = pl.pallas_call(
        functools.partial(pack_kernel, swaps),
        out_shape=[jax.ShapeDtypeStruct(shape, jnp.int32) for shape in shapes],
        in_specs=[VMEM],
        out_specs=[VMEM] * len(swaps),
        compiler_params=PARAMS,
        cost_estimate=cost(1 << 20),
        name="pack",
    )(volume)
    received = [
        lax.ppermute(message, AXES, swap_pairs(sizes, axis, step))
        for (axis, step), message in zip(swaps, messages)
    ]

    image = jax.ShapeDtypeStruct((4, rows, cols), jnp.float32)
    partial = pl.pallas_call(
        functools.partial(march_kernel, swaps, sizes, extent),
        out_shape=image,
        in_specs=[VMEM, VMEM, SMEM] + [VMEM] * len(swaps),
        out_specs=VMEM,
        compiler_params=PARAMS,
        cost_estimate=cost(1 << 22),
        name="march",
    )(volume, transfer_table, footprint.reshape(4), *received)

    count = sizes[0]
    layers = [partial] + [
        lax.ppermute(partial, AXES[0], [((i + k) % count, i) for i in range(count)]) for k in range(1, count)
    ]
    return pl.pallas_call(
        functools.partial(blend_kernel, count),
        out_shape=image,
        in_specs=[SMEM] + [VMEM] * count,
        out_specs=VMEM,
        compiler_params=PARAMS,
        cost_estimate=cost(1 << 20),
        name="blend",
    )(depth_rank, *layers)


def solution(mesh):
    placed = (P("gx", "gy", "gz"), P(), P(), P("gx", "gy", "gz", None))
    return jax.shard_map(
        on_device, mesh=mesh, in_specs=placed, out_specs=P(None, "gy", "gz"), check_vma=False
    )
```
